32 devices in a mesh: dp: 8 (over y, x, core), fsdp: 4 (over z).
Axes of the slice: x: 2, y: 2, z: 4, core: 2. Of those that a mesh axis runs over, the one named last changes fastest.
Arguments:
- tokens: bfloat16 [64, 512, 768], P(('dp', 'fsdp')), may hold values from -6 to 6
- lengths: int32 [64], P(('dp', 'fsdp')), may hold values from 1 to 512, 24576 in all
- cotangent: bfloat16 [64, 512, 768], P(('dp', 'fsdp')), may hold values from -6 to 6
- w_query: bfloat16 [768, 768], P(('dp', 'fsdp')), may hold values from -0.21875 to 0.21875
- w_key: bfloat16 [768, 768], P(('dp', 'fsdp')), may hold values from -0.21875 to 0.21875
- w_value: bfloat16 [768, 768], P(('dp', 'fsdp')), may hold values from -0.21875 to 0.21875
- w_out: bfloat16 [768, 768], P(('dp', 'fsdp')), may hold values from -0.875 to 0.875
- w_up: bfloat16 [768, 3072], P(('dp', 'fsdp')), may hold values from -0.21875 to 0.21875
- w_down: bfloat16 [3072, 768], P(('dp', 'fsdp')), may hold values from -0.109375 to 0.109375
- shared_a: bfloat16 [768, 1024], P(('dp', 'fsdp')), may hold values from -0.21875 to 0.21875
- shared_b: bfloat16 [1024, 768], P(('dp', 'fsdp')), may hold values from -0.1875 to 0.1875
- gain_one: float32 [768], replicated, may hold values from 0.5 to 1.5
- gain_two: float32 [768], replicated, may hold values from 0.5 to 1.5
- query_d: float32 [1024], replicated, may hold values from -4 to 4
- query_b: float32 [768], replicated, may hold values from -4 to 4
- value_d: float32 [1024], replicated, may hold values from -4 to 4
- value_b: float32 [768], replicated, may hold values from -4 to 4
Outputs:
- output: bfloat16 [64, 512, 768], P(('dp', 'fsdp'))
- grad_tokens: bfloat16 [64, 512, 768], P(('dp', 'fsdp'))
- grad_query_d: float32 [1024], replicated
- grad_query_b: float32 [768], replicated
- grad_value_d: float32 [1024], replicated
- grad_value_b: float32 [768], replicated
- rank_stats: float32 [1024], replicated
The draws below stay inside these ranges and needn't reach their ends.
Inputs may be any that keep to these rules, and one draw needn't show every extreme that they name: The 64 lengths sum to 24576, and the largest equals 512.
All inputs are finite; a program needn't handle non-finite values. No bound on the sum of `lengths` on one device may be relied on, other than what follows from the above.
Results may differ from the reference program's by a relative error of at most 0.015.
The reference program's roundings to bfloat16 on the way count: a program that leaves them out, or rounds other values in their place, can miss the bound.
Values may be sent and summed in bfloat16 or wider, within the bound.
A program may use at most 192 MiB of HBM per device.

```python
import math
import jax
import jax.numpy as jnp
import numpy as np
from jax import lax

D = 768
H = 12
HD = 64
FF = 3072
R = 1024
L = 512
SEQS = 64


def level_of(key, dims, shards, smallest, high):
    level = 1.0
    for axis_at, blocks in shards:
        steps = jax.random.uniform(jax.random.fold_in(jax.random.fold_in(key, 6), axis_at), (blocks,), jnp.float32, smallest / len(shards), high / len(shards))
        level = level * jnp.repeat(jnp.exp(steps), dims[axis_at] // blocks).reshape((-1,) + (1,) * (len(dims) - 1 - axis_at))
    return level


def profile(number_of, total, bound, lean):
    portions = [(1 << 20) // math.isqrt(rank ** lean) + 1 for rank in range(2, number_of + 1)]
    spare, given = total - bound - (number_of - 1), [1] * (number_of - 1)
    while spare > 0:
        free = [i for i in range(number_of - 1) if given[i] < bound]
        whole, remaining = sum([portions[i] for i in free]), spare
        for i in free:
            addition = min(bound - given[i], max(1, remaining * portions[i] // whole), spare)
            given[i] = given[i] + addition
            spare = spare - addition
    return np.array([bound] + given)


def uneven_parts(rng, count, total, reach, slope):
    if count == 2:
        one = jax.random.randint(rng, (), max(1, total - reach), min(reach, total - 1) + 1)
        return jnp.stack([one, total - one])
    sizes = jnp.asarray(profile(count, total, reach, slope), jnp.int32)
    couples = (count - 1) // 2
    giver, sink = sizes[1:1 + 2 * couples:2], sizes[2:2 + 2 * couples:2]
    slack = jnp.minimum(giver - 1, reach - sink)
    passed = jax.random.randint(jax.random.fold_in(rng, 1), (couples,), 0, 1 << 20) % (slack + 1)
    sizes = sizes.at[1:1 + 2 * couples:2].set(giver - passed).at[2:2 + 2 * couples:2].set(sink + passed)
    return sizes[jax.random.permutation(jax.random.fold_in(rng, 2), count)]


def noise(rng, dims, width, most, cuts=(), kind=jnp.bfloat16):
    values = jax.random.normal(rng, dims, jnp.float32) * width
    if len(cuts) > 0:
        values = level_of(rng, dims, cuts, -0.22, 0.18) * values
    return jnp.clip(values, min=-most, max=most).astype(kind)


def setup_inputs(seed: int = 0) -> dict:
    streams_of = jax.random.split(jax.random.key(seed), 18)
    return {
        "tokens": noise(streams_of[0], (SEQS, L, D), 1.0, 6.0, ((0, 32),)),
        "lengths": uneven_parts(streams_of[1], SEQS, SEQS * L * 3 // 4, L, 2).astype(jnp.int32),
        "cotangent": noise(streams_of[2], (SEQS, L, D), 1.0, 6.0, ((0, 32),)),
        "w_query": noise(streams_of[3], (D, D), D ** -0.5, 0.21875, ((0, 32),)),
        "w_key": noise(streams_of[4], (D, D), D ** -0.5, 0.21875, ((0, 32),)),
        "w_value": noise(streams_of[5], (D, D), D ** -0.5, 0.21875, ((0, 32),)),
        "w_out": noise(streams_of[6], (D, D), (D // 16) ** -0.5, 0.875, ((0, 32),)),
        "w_up": noise(streams_of[7], (D, FF), D ** -0.5, 0.21875, ((0, 32),)),
        "w_down": noise(streams_of[8], (FF, D), FF ** -0.5, 0.109375, ((0, 32),)),
        "shared_a": noise(streams_of[9], (D, R), D ** -0.5, 0.21875, ((0, 32),)),
        "shared_b": noise(streams_of[10], (R, D), R ** -0.5, 0.1875, ((0, 32),)),
        "gain_one": jnp.clip(1.0 + 0.1 * jax.random.normal(streams_of[11], (D,), jnp.float32), 0.5, 1.5),
        "gain_two": jnp.clip(1.0 + 0.1 * jax.random.normal(streams_of[12], (D,), jnp.float32), 0.5, 1.5),
        "query_d": noise(streams_of[13], (R,), 1.0, 4.0, (), jnp.float32),
        "query_b": noise(streams_of[14], (D,), 1.0, 4.0, (), jnp.float32),
        "value_d": noise(streams_of[15], (R,), 1.0, 4.0, (), jnp.float32),
        "value_b": noise(streams_of[16], (D,), 1.0, 4.0, (), jnp.float32),
    }


@jax.custom_vjp
def low(v):
    return lax.optimization_barrier(v.astype(jnp.bfloat16)).astype(jnp.float32)

@jax.custom_vjp
def low_back(v):
    return v

def low_keep(v):
    return (low(v), None)

def low_pass(kept, grad):
    return (grad,)

def back_keep(v):
    return (v, None)

def back_low(kept, grad):
    return (low(grad),)
low.defvjp(low_keep, low_pass)
low_back.defvjp(back_keep, back_low)
eps_norm = 1e-05
neg_fill = -1000000000.0

def product(left, right):
    return jnp.dot(left, right, precision=lax.Precision.HIGHEST, preferred_element_type=jnp.float32)

def layer_norm(hidden, gain):
    center = lax.optimization_barrier(jnp.mean(hidden, axis=-1, keepdims=True))
    shifted = hidden - center
    spread = lax.optimization_barrier(jnp.mean(shifted * shifted, axis=-1, keepdims=True))
    return shifted * lax.rsqrt(spread + eps_norm) * gain

def attend(queries, key_rows, values, length):
    q_heads = queries.reshape(L, H, HD)
    k_heads = key_rows.reshape(L, H, HD)
    v_heads = values.reshape(L, H, HD)
    scores = jnp.einsum('qhd,khd->hqk', q_heads, k_heads, precision=lax.Precision.HIGHEST) * HD ** (-0.5)
    key_live = lax.broadcasted_iota(jnp.int32, (1, 1, L), 2) < length
    scores = jnp.where(key_live, low_back(scores), neg_fill)
    row_max = lax.optimization_barrier(jnp.max(scores, axis=-1, keepdims=True))
    log_total = row_max + jnp.log(lax.optimization_barrier(jnp.sum(jnp.exp(scores - row_max), axis=-1, keepdims=True)))
    probs = low(jnp.exp(scores - log_total))
    context = jnp.einsum('hqk,khd->qhd', probs, v_heads, precision=lax.Precision.HIGHEST)
    return context.reshape(L, D)

def reference(tokens, lengths, cotangent, w_query, w_key, w_value, w_out, w_up, w_down, shared_a, shared_b, gain_one, gain_two, query_d, query_b, value_d, value_b):
    wq, wk, wv, wo, wu, wd, mat_a, mat_b = [m.astype(jnp.float32) for m in (w_query, w_key, w_value, w_out, w_up, w_down, shared_a, shared_b)]
    per_step = 8
    steps_count = SEQS // per_step
    positions = lax.broadcasted_iota(jnp.int32, (SEQS, L), 1)
    live = (positions < lengths[:, None]).astype(jnp.float32)
    token_all = tokens.astype(jnp.float32).reshape(steps_count, per_step, L, D)
    cot_all = (cotangent.astype(jnp.float32) * live[:, :, None]).reshape(steps_count, per_step, L, D)
    live_all = live.reshape(steps_count, per_step, L)
    length_all = lengths.reshape(steps_count, per_step)

    def forward(inputs, vec_qd, vec_qb, vec_vd, vec_vb, group_len):
        rank_act = low_back(product(inputs, mat_a))
        rank_q = low(rank_act * vec_qd)
        rank_v = low(rank_act * vec_vd)
        delta_q = low_back(product(rank_q, mat_b))
        delta_v = low_back(product(rank_v, mat_b))
        queries = low(low_back(product(inputs, wq) + vec_qb * delta_q))
        key_rows = low(low_back(product(inputs, wk)))
        values = low(low_back(product(inputs, wv) + vec_vb * delta_v))
        context = lax.map(lambda parts: jax.checkpoint(attend)(*parts), (queries, key_rows, values, group_len))
        context = low(low_back(context))
        h_one = inputs + low_back(product(context, wo))
        x_one = layer_norm(h_one, gain_one)
        pre_act = low_back(product(low(x_one), wu))
        act = low(jax.nn.gelu(pre_act, approximate=False))
        h_two = x_one + low_back(product(act, wd))
        return layer_norm(h_two, gain_two)

    def one_group(carry, pieces):
        inputs, cot_rows, live_rows, group_len = pieces
        outputs, pull_back = jax.vjp(lambda a, b, c, e, f: forward(a, b, c, e, f, group_len), inputs, query_d, query_b, value_d, value_b)
        g_in, g_qd, g_qb, g_vd, g_vb = pull_back(cot_rows)
        rank_act = product(inputs, mat_a)
        square_sum = lax.optimization_barrier(jnp.sum(rank_act * rank_act * live_rows[:, :, None], axis=(0, 1)))
        carry = (carry[0] + g_qd, carry[1] + g_qb, carry[2] + g_vd, carry[3] + g_vb, carry[4] + square_sum)
        return (carry, (outputs.astype(jnp.bfloat16), g_in.astype(jnp.bfloat16)))
    zero_r = jnp.zeros((R,), jnp.float32)
    zero_d = jnp.zeros((D,), jnp.float32)
    totals, results = lax.scan(one_group, (zero_r, zero_d, zero_r, zero_d, zero_r), (token_all, cot_all, live_all, length_all))
    output = results[0].reshape(SEQS, L, D)
    grad_tokens = results[1].reshape(SEQS, L, D)
    count = jnp.sum(lengths.astype(jnp.float32))
    rank_stats = totals[4] / count
    return (output, grad_tokens, totals[0], totals[1], totals[2], totals[3], rank_stats)
```

```python
import functools
import jax
import jax.numpy as jnp
from jax import lax
from jax.experimental import pallas as pl
from jax.experimental.pallas import tpu as pltpu

D = 768
H = 12
HD = 64
FF = 3072
R = 1024
L = 512
eps_norm = 1e-05
neg_fill = -1000000000.0
f32 = jnp.float32
bf16 = jnp.bfloat16


def mm(a, b):
    return jnp.dot(a, b, preferred_element_type=f32)


def mm_t(a, b):
    return lax.dot_general(a, b, (((1,), (1,)), ((), ())), preferred_element_type=f32)


def fold8(z):
    rows, cols = z.shape
    return jnp.sum(z.reshape(rows // 8, 8, cols), axis=0)


def vm(mib):
    return pltpu.CompilerParams(vmem_limit_bytes=mib << 20)


def proj_kernel(tm, len_ref, x_ref, w1_ref, b_ref, qd_ref, vd_ref, qb_ref, vb_ref,
                ra_ref, dq_ref, dv_ref, q_ref, k_ref, v_ref, sq_ref):
    i = pl.program_id(0)
    x = x_ref[...]
    ra = mm(x, w1_ref[:, :R])
    per_seq = L // tm
    length = len_ref[i // per_seq]
    pos = (i % per_seq) * tm + lax.broadcasted_iota(jnp.int32, (tm, 1), 0)
    live = (pos < length).astype(f32)

    @pl.when(i == 0)
    def _():
        sq_ref[...] = jnp.zeros_like(sq_ref)

    sq_ref[...] += fold8(ra * ra * live)
    ra_ref[...] = ra.astype(ra_ref.dtype)
    rank_q = (ra * qd_ref[...]).astype(bf16)
    rank_v = (ra * vd_ref[...]).astype(bf16)
    delta_q = mm(rank_q, b_ref[...])
    dq_ref[...] = delta_q.astype(dq_ref.dtype)
    q = (mm(x, w1_ref[:, R:R + D]) + qb_ref[...] * delta_q).astype(bf16)
    q_ref[...] = q * (HD ** -0.5)
    delta_v = mm(rank_v, b_ref[...])
    dv_ref[...] = delta_v.astype(dv_ref.dtype)
    v_ref[...] = (mm(x, w1_ref[:, R + 2 * D:]) + vb_ref[...] * delta_v).astype(bf16)
    k_ref[...] = mm(x, w1_ref[:, R + D:R + 2 * D]).astype(bf16)


def proj(lengths, x, w1, b, qd, vd, qb, vb, tm=256):
    n = x.shape[0]
    row = lambda c: pl.BlockSpec((tm, c), lambda i, *_: (i, 0))
    full = lambda a: pl.BlockSpec(a.shape, lambda i, *_: (0, 0), pipeline_mode=pl.Buffered(1))
    sd = jax.ShapeDtypeStruct
    return pl.pallas_call(
        functools.partial(proj_kernel, tm),
        grid_spec=pltpu.PrefetchScalarGridSpec(
            num_scalar_prefetch=1, grid=(n // tm,),
            in_specs=[row(D), full(w1), full(b)] + [full(a) for a in (qd, vd, qb, vb)],
            out_specs=[row(R), row(D), row(D), row(D), row(D), row(D),
                       pl.BlockSpec((8, R), lambda i, *_: (0, 0))]),
        out_shape=[sd((n, R), bf16), sd((n, D), bf16), sd((n, D), bf16), sd((n, D), bf16),
                   sd((n, D), bf16), sd((n, D), bf16), sd((8, R), f32)],
        name="proj",
        compiler_params=vm(48),
    )(lengths, x, w1, b, qd, vd, qb, vb)


def attn_fwd_kernel(len_ref, q_ref, k_ref, v_ref, ctx_ref, p_ref):
    s = pl.program_id(0)
    length = len_ref[s]
    live = lax.broadcasted_iota(jnp.int32, (L, 1), 0) < length
    lane = lax.broadcasted_iota(jnp.int32, (L, 2 * HD), 1)
    q = q_ref[...]
    k = k_ref[...]
    v = v_ref[...]
    zero = jnp.zeros_like(k)
    vt = v.T
    parts = []
    for h in range(2):
        kh = jnp.where((lane // HD) == h, k, zero)
        st = mm_t(kh, q)
        st = jnp.where(live, st, neg_fill)
        top = jnp.max(st, axis=0, keepdims=True)
        e = jnp.exp(st - top)
        total = jnp.sum(e, axis=0, keepdims=True)
        pt = (e * (1.0 / total)).astype(bf16)
        p_ref[h] = pt
        parts.append(mm(vt[h * HD:(h + 1) * HD], pt))
    ctx_ref[...] = jnp.concatenate(parts, axis=0).astype(bf16).T


def attn_fwd(lengths, q, k, v):
    n = q.shape[0]
    seqs = n // L
    pairs = H // 2
    blk = pl.BlockSpec((L, 2 * HD), lambda s, h, *_: (s, h))
    sd = jax.ShapeDtypeStruct
    return pl.pallas_call(
        attn_fwd_kernel,
        grid_spec=pltpu.PrefetchScalarGridSpec(
            num_scalar_prefetch=1, grid=(seqs, pairs),
            in_specs=[blk, blk, blk],
            out_specs=[blk, pl.BlockSpec((2, L, L), lambda s, h, *_: (s * pairs + h, 0, 0))]),
        out_shape=[sd((n, D), bf16), sd((seqs * H, L, L), bf16)],
        name="attn_fwd",
        compiler_params=vm(48),
    )(lengths, q, k, v)


def ffn_kernel(tm, cj, len_ref, x_ref, ctx_ref, cot_ref, w2_ref, wd_ref, g1_ref, g2_ref,
               out_ref, gh1_ref, gctx_ref, dg_ref, acc_ref):
    i = pl.program_id(0)
    n_j = FF // cj
    g1 = g1_ref[...]
    g2 = g2_ref[...]
    h1 = x_ref[...].astype(f32) + mm(ctx_ref[...], w2_ref[:, :D])
    c1 = h1 - jnp.mean(h1, axis=-1, keepdims=True)
    r1 = lax.rsqrt(jnp.mean(c1 * c1, axis=-1, keepdims=True) + eps_norm)
    y1 = c1 * r1
    x1 = y1 * g1
    x_low = x1.astype(bf16)
    acc_ref[...] = x1

    def fwd(j, carry):
        wu = w2_ref[:, pl.ds(pl.multiple_of(D + j * cj, 128), cj)]
        pre = mm(x_low, wu)
        cdf = 0.5 + 0.5 * lax.erf(pre * (0.5 ** 0.5))
        pdf = jnp.exp(pre * pre * -0.5) * 0.3989422804014327
        act = (pre * cdf).astype(bf16)
        dg_ref[j] = (cdf + pre * pdf).astype(bf16)
        acc_ref[...] += mm(act, wd_ref[pl.ds(pl.multiple_of(j * cj, 128), cj), :])
        return carry

    lax.fori_loop(0, n_j, fwd, 0)
    h2 = acc_ref[...]
    c2 = h2 - jnp.mean(h2, axis=-1, keepdims=True)
    r2 = lax.rsqrt(jnp.mean(c2 * c2, axis=-1, keepdims=True) + eps_norm)
    y2 = c2 * r2
    out_ref[...] = (y2 * g2).astype(bf16)
    per_seq = L // tm
    length = len_ref[i // per_seq]
    pos = (i % per_seq) * tm + lax.broadcasted_iota(jnp.int32, (tm, 1), 0)
    live = (pos < length).astype(f32)
    gy = cot_ref[...].astype(f32) * live * g2
    gh2 = (gy - jnp.mean(gy, axis=-1, keepdims=True)
           - y2 * jnp.mean(gy * y2, axis=-1, keepdims=True)) * r2
    g_ffn = gh2.astype(bf16)
    acc_ref[...] = gh2

    def bwd(j, carry):
        wd = wd_ref[pl.ds(pl.multiple_of(j * cj, 128), cj), :]
        g_act = mm_t(g_ffn, wd)
        g_pre = (dg_ref[j].astype(f32) * g_act).astype(bf16)
        wu = w2_ref[:, pl.ds(pl.multiple_of(D + j * cj, 128), cj)]
        acc_ref[...] += mm_t(g_pre, wu)
        return carry

    lax.fori_loop(0, n_j, bwd, 0)
    gx1 = acc_ref[...]
    gy1 = gx1 * g1
    gh1 = (gy1 - jnp.mean(gy1, axis=-1, keepdims=True)
           - y1 * jnp.mean(gy1 * y1, axis=-1, keepdims=True)) * r1
    gh1_ref[...] = gh1
    gctx_ref[...] = mm_t(gh1.astype(bf16), w2_ref[:, :D]).astype(bf16)


def ffn(lengths, x, ctx, cot, w2, wd, g1, g2, tm=256, cj=768):
    n = x.shape[0]
    row = pl.BlockSpec((tm, D), lambda i, *_: (i, 0))
    full = lambda a: pl.BlockSpec(a.shape, lambda i, *_: (0, 0), pipeline_mode=pl.Buffered(1))
    sd = jax.ShapeDtypeStruct
    return pl.pallas_call(
        functools.partial(ffn_kernel, tm, cj),
        grid_spec=pltpu.PrefetchScalarGridSpec(
            num_scalar_prefetch=1, grid=(n // tm,),
            in_specs=[row, row, row, full(w2), full(wd), full(g1), full(g2)],
            out_specs=[row, row, row],
            scratch_shapes=[pltpu.VMEM((FF // cj, tm, cj), bf16), pltpu.VMEM((tm, D), f32)]),
        out_shape=[sd((n, D), bf16), sd((n, D), f32), sd((n, D), bf16)],
        name="ffn",
        compiler_params=vm(56),
    )(lengths, x, ctx, cot, w2, wd, g1, g2)


def attn_bwd_kernel(q_ref, k_ref, v_ref, ctx_ref, gc_ref, p_ref, gq_ref, gk_ref, gv_ref):
    lane = lax.broadcasted_iota(jnp.int32, (L, 2 * HD), 1)
    q = q_ref[...]
    k = k_ref[...]
    v = v_ref[...]
    gc = gc_ref[...]
    zero = jnp.zeros_like(k)
    prod = (gc.astype(f32) * ctx_ref[...].astype(f32)).T
    kt = k.T
    gq_parts = []
    gk = jnp.zeros((L, 2 * HD), f32)
    gv = jnp.zeros((L, 2 * HD), f32)
    for h in range(2):
        mine = (lane // HD) == h
        vh = jnp.where(mine, v, zero)
        qh = jnp.where(mine, q, zero)
        gch = jnp.where(mine, gc, zero)
        pt = p_ref[h]
        gpt = mm_t(vh, gc)
        row = jnp.sum(prod[h * HD:(h + 1) * HD], axis=0, keepdims=True)
        gst = (pt.astype(f32) * (gpt - row)).astype(bf16)
        gq_parts.append(mm(kt[h * HD:(h + 1) * HD], gst))
        gk += mm(gst, qh)
        gv += mm(pt, gch)
    gq = jnp.concatenate(gq_parts, axis=0) * (HD ** -0.5)
    gq_ref[...] = gq.astype(bf16).T
    gk_ref[...] = gk.astype(bf16)
    gv_ref[...] = gv.astype(bf16)


def attn_bwd(q, k, v, ctx, gc, p):
    n = q.shape[0]
    seqs = n // L
    pairs = H // 2
    blk = pl.BlockSpec((L, 2 * HD), lambda s, h: (s, h))
    sd = jax.ShapeDtypeStruct
    return pl.pallas_call(
        attn_bwd_kernel,
        grid=(seqs, pairs),
        in_specs=[blk] * 5 + [pl.BlockSpec((2, L, L), lambda s, h: (s * pairs + h, 0, 0))],
        out_specs=[blk] * 3,
        out_shape=[sd((n, D), bf16)] * 3,
        name="attn_bwd",
        compiler_params=vm(48),
    )(q, k, v, ctx, gc, p)


def grads_kernel(gq_ref, gk_ref, gv_ref, dq_ref, dv_ref, ra_ref, gh1_ref, w1_ref, b_ref,
                 qd_ref, vd_ref, qb_ref, vb_ref, gt_ref, sqd_ref, svd_ref, sqb_ref, svb_ref):
    i = pl.program_id(0)

    @pl.when(i == 0)
    def _():
        for ref in (sqd_ref, svd_ref, sqb_ref, svb_ref):
            ref[...] = jnp.zeros_like(ref)

    gq = gq_ref[...].astype(f32)
    gv = gv_ref[...].astype(f32)
    ra = ra_ref[...].astype(f32)
    sqb_ref[...] += fold8(gq * dq_ref[...].astype(f32))
    svb_ref[...] += fold8(gv * dv_ref[...].astype(f32))
    t_q = mm_t((qb_ref[...] * gq).astype(bf16), b_ref[...])
    t_v = mm_t((vb_ref[...] * gv).astype(bf16), b_ref[...])
    sqd_ref[...] += fold8(t_q * ra)
    svd_ref[...] += fold8(t_v * ra)
    g_rank = (t_q * qd_ref[...] + t_v * vd_ref[...]).astype(bf16)
    acc = gh1_ref[...].astype(f32)
    acc += mm_t(gq_ref[...], w1_ref[:, R:R + D])
    acc += mm_t(gk_ref[...], w1_ref[:, R + D:R + 2 * D])
    acc += mm_t(gv_ref[...], w1_ref[:, R + 2 * D:])
    acc += mm_t(g_rank, w1_ref[:, :R])
    gt_ref[...] = acc.astype(bf16)


def grads(gq, gk, gv, dq, dv, ra, gh1, w1, b, qd, vd, qb, vb, tm=256):
    n = gq.shape[0]
    row = lambda c: pl.BlockSpec((tm, c), lambda i: (i, 0))
    full = lambda a: pl.BlockSpec(a.shape, lambda i: (0, 0), pipeline_mode=pl.Buffered(1))
    acc = lambda c: pl.BlockSpec((8, c), lambda i: (0, 0))
    sd = jax.ShapeDtypeStruct
    return pl.pallas_call(
        grads_kernel,
        grid=(n // tm,),
        in_specs=[row(D)] * 5 + [row(R), row(D), full(w1), full(b)] + [full(a) for a in (qd, vd, qb, vb)],
        out_specs=[row(D), acc(R), acc(R), acc(D), acc(D)],
        out_shape=[sd((n, D), bf16), sd((8, R), f32), sd((8, R), f32), sd((8, D), f32), sd((8, D), f32)],
        name="grads",
        compiler_params=vm(48),
    )(gq, gk, gv, dq, dv, ra, gh1, w1, b, qd, vd, qb, vb)


def shards(
    tokens,
    lengths,
    cotangent,
    w_query,
    w_key,
    w_value,
    w_out,
    w_up,
    w_down,
    shared_a,
    shared_b,
    gain_one,
    gain_two,
    query_d,
    query_b,
    value_d,
    value_b,
):
    axes = ("dp", "fsdp")
    seqs = tokens.shape[0]
    x = tokens.reshape(seqs * L, D)
    cot = cotangent.reshape(seqs * L, D)
    gather = lambda a: lax.all_gather(a, axes, axis=0, tiled=True)
    w1 = gather(jnp.concatenate([shared_a, w_query, w_key, w_value], axis=1))
    b = gather(shared_b)
    w2 = gather(jnp.concatenate([w_out, w_up], axis=1))
    wd = gather(w_down)
    g1, g2, qd, qb, vd, vb = (
        a.reshape(1, -1) for a in (gain_one, gain_two, query_d, query_b, value_d, value_b)
    )
    ra, dq, dv, q, k, v, sq = proj(lengths, x, w1, b, qd, vd, qb, vb)
    ctx, p = attn_fwd(lengths, q, k, v)
    out, gh1, gc = ffn(lengths, x, ctx, cot, w2, wd, g1, g2)
    gq, gk, gv = attn_bwd(q, k, v, ctx, gc, p)
    gt, s_qd, s_vd, s_qb, s_vb = grads(gq, gk, gv, dq, dv, ra, gh1, w1, b, qd, vd, qb, vb)
    count = jnp.sum(lengths).astype(f32)
    sums = tuple(jnp.sum(a, axis=0) for a in (s_qd, s_qb, s_vd, s_vb, sq))
    s_qd, s_qb, s_vd, s_vb, sq, count = lax.psum(sums + (count,), axes)
    return (out.reshape(seqs, L, D), gt.reshape(seqs, L, D), s_qd, s_qb, s_vd, s_vb, sq / count)


def solution(mesh):
    from jax.sharding import PartitionSpec as P

    both = ("dp", "fsdp")
    mat = P(both, None)
    big = P(both, None, None)
    in_specs = (big, P(both), big) + (mat,) * 8 + (P(),) * 6
    out_specs = (big, big) + (P(),) * 5
    return jax.shard_map(shards, mesh=mesh, in_specs=in_specs, out_specs=out_specs, check_vma=False)
```

```python
import functools
import jax
import jax.numpy as jnp
from jax import lax
from jax.experimental import pallas as pl
from jax.experimental.pallas import tpu as pltpu

D = 768
H = 12
HD = 64
FF = 3072
R = 1024
L = 512
eps_norm = 1e-05
neg_fill = -1000000000.0
f32 = jnp.float32
bf16 = jnp.bfloat16


def mm(a, b):
    return jnp.dot(a, b, preferred_element_type=f32)


def mm_t(a, b):
    return lax.dot_general(a, b, (((1,), (1,)), ((), ())), preferred_element_type=f32)


def fold8(z):
    rows, cols = z.shape
    return jnp.sum(z.reshape(rows // 8, 8, cols), axis=0)


def vm(mib):
    return pltpu.CompilerParams(vmem_limit_bytes=mib << 20)


def proj_kernel(tm, len_ref, x_ref, w1_ref, b_ref, qd_ref, vd_ref, qb_ref, vb_ref,
                ra_ref, dq_ref, dv_ref, q_ref, k_ref, v_ref, sq_ref):
    i = pl.program_id(0)
    x = x_ref[...]
    ra = mm(x, w1_ref[:, :R])
    per_seq = L // tm
    length = len_ref[i // per_seq]
    pos = (i % per_seq) * tm + lax.broadcasted_iota(jnp.int32, (tm, 1), 0)
    live = (pos < length).astype(f32)

    @pl.when(i == 0)
    def _():
        sq_ref[...] = jnp.zeros_like(sq_ref)

    sq_ref[...] += fold8(ra * ra * live)
    ra_ref[...] = ra.astype(ra_ref.dtype)
    rank_q = (ra * qd_ref[...]).astype(bf16)
    rank_v = (ra * vd_ref[...]).astype(bf16)
    delta_q = mm(rank_q, b_ref[...])
    dq_ref[...] = delta_q.astype(dq_ref.dtype)
    q = (mm(x, w1_ref[:, R:R + D]) + qb_ref[...] * delta_q).astype(bf16)
    q_ref[...] = q * (HD ** -0.5)
    delta_v = mm(rank_v, b_ref[...])
    dv_ref[...] = delta_v.astype(dv_ref.dtype)
    v_ref[...] = (mm(x, w1_ref[:, R + 2 * D:]) + vb_ref[...] * delta_v).astype(bf16)
    k_ref[...] = mm(x, w1_ref[:, R + D:R + 2 * D]).astype(bf16)


def proj(lengths, x, w1, b, qd, vd, qb, vb, tm=256):
    n = x.shape[0]
    row = lambda c: pl.BlockSpec((tm, c), lambda i, *_: (i, 0))
    full = lambda a: pl.BlockSpec(a.shape, lambda i, *_: (0, 0), pipeline_mode=pl.Buffered(1))
    sd = jax.ShapeDtypeStruct
    return pl.pallas_call(
        functools.partial(proj_kernel, tm),
        grid_spec=pltpu.PrefetchScalarGridSpec(
            num_scalar_prefetch=1, grid=(n // tm,),
            in_specs=[row(D), full(w1), full(b)] + [full(a) for a in (qd, vd, qb, vb)],
            out_specs=[row(R), row(D), row(D), row(D), row(D), row(D),
                       pl.BlockSpec((8, R), lambda i, *_: (0, 0))]),
        out_shape=[sd((n, R), bf16), sd((n, D), bf16), sd((n, D), bf16), sd((n, D), bf16),
                   sd((n, D), bf16), sd((n, D), bf16), sd((8, R), f32)],
        name="proj",
        compiler_params=vm(48),
    )(lengths, x, w1, b, qd, vd, qb, vb)


def attn_fwd_kernel(len_ref, q_ref, k_ref, v_ref, ctx_ref, p_ref):
    s = pl.program_id(0)
    length = len_ref[s]
    live = lax.broadcasted_iota(jnp.int32, (L, 1), 0) < length
    lane = lax.broadcasted_iota(jnp.int32, (L, 2 * HD), 1)
    q = q_ref[...]
    k = k_ref[...]
    v = v_ref[...]
    zero = jnp.zeros_like(k)
    vt = v.T
    parts = []
    for h in range(2):
        kh = jnp.where((lane // HD) == h, k, zero)
        st = mm_t(kh, q)
        st = jnp.where(live, st, neg_fill)
        top = jnp.max(st, axis=0, keepdims=True)
        e = jnp.exp(st - top)
        total = jnp.sum(e, axis=0, keepdims=True)
        pt = (e * (1.0 / total)).astype(bf16)
        p_ref[h] = pt
        parts.append(mm(vt[h * HD:(h + 1) * HD], pt))
    ctx_ref[...] = jnp.concatenate(parts, axis=0).astype(bf16).T


def attn_fwd(lengths, q, k, v):
    n = q.shape[0]
    seqs = n // L
    pairs = H // 2
    blk = pl.BlockSpec((L, 2 * HD), lambda s, h, *_: (s, h))
    sd = jax.ShapeDtypeStruct
    return pl.pallas_call(
        attn_fwd_kernel,
        grid_spec=pltpu.PrefetchScalarGridSpec(
            num_scalar_prefetch=1, grid=(seqs, pairs),
            in_specs=[blk, blk, blk],
            out_specs=[blk, pl.BlockSpec((2, L, L), lambda s, h, *_: (s * pairs + h, 0, 0))]),
        out_shape=[sd((n, D), bf16), sd((seqs * H, L, L), bf16)],
        name="attn_fwd",
        compiler_params=vm(48),
    )(lengths, q, k, v)


def ffn_kernel(tm, cj, len_ref, x_ref, ctx_ref, cot_ref, w2_ref, wd_ref, g1_ref, g2_ref,
               out_ref, gh1_ref, gctx_ref, dg_ref, acc_ref):
    i = pl.program_id(0)
    n_j = FF // cj
    g1 = g1_ref[...]
    g2 = g2_ref[...]
    h1 = x_ref[...].astype(f32) + mm(ctx_ref[...], w2_ref[:, :D])
    c1 = h1 - jnp.mean(h1, axis=-1, keepdims=True)
    r1 = lax.rsqrt(jnp.mean(c1 * c1, axis=-1, keepdims=True) + eps_norm)
    y1 = c1 * r1
    x1 = y1 * g1
    x_low = x1.astype(bf16)
    acc_ref[...] = x1

    def fwd(j, carry):
        wu = w2_ref[:, pl.ds(pl.multiple_of(D + j * cj, 128), cj)]
        pre = mm(x_low, wu)
        cdf = 0.5 + 0.5 * lax.erf(pre * (0.5 ** 0.5))
        pdf = jnp.exp(pre * pre * -0.5) * 0.3989422804014327
        act = (pre * cdf).astype(bf16)
        dg_ref[j] = (cdf + pre * pdf).astype(bf16)
        acc_ref[...] += mm(act, wd_ref[pl.ds(pl.multiple_of(j * cj, 128), cj), :])
        return carry

    lax.fori_loop(0, n_j, fwd, 0)
    h2 = acc_ref[...]
    c2 = h2 - jnp.mean(h2, axis=-1, keepdims=True)
    r2 = lax.rsqrt(jnp.mean(c2 * c2, axis=-1, keepdims=True) + eps_norm)
    y2 = c2 * r2
    out_ref[...] = (y2 * g2).astype(bf16)
    per_seq = L // tm
    length = len_ref[i // per_seq]
    pos = (i % per_seq) * tm + lax.broadcasted_iota(jnp.int32, (tm, 1), 0)
    live = (pos < length).astype(f32)
    gy = cot_ref[...].astype(f32) * live * g2
    gh2 = (gy - jnp.mean(gy, axis=-1, keepdims=True)
           - y2 * jnp.mean(gy * y2, axis=-1, keepdims=True)) * r2
    g_ffn = gh2.astype(bf16)
    acc_ref[...] = gh2

    def bwd(j, carry):
        wd = wd_ref[pl.ds(pl.multiple_of(j * cj, 128), cj), :]
        g_act = mm_t(g_ffn, wd)
        g_pre = (dg_ref[j].astype(f32) * g_act).astype(bf16)
        wu = w2_ref[:, pl.ds(pl.multiple_of(D + j * cj, 128), cj)]
        acc_ref[...] += mm_t(g_pre, wu)
        return carry

    lax.fori_loop(0, n_j, bwd, 0)
    gx1 = acc_ref[...]
    gy1 = gx1 * g1
    gh1 = (gy1 - jnp.mean(gy1, axis=-1, keepdims=True)
           - y1 * jnp.mean(gy1 * y1, axis=-1, keepdims=True)) * r1
    gh1_ref[...] = gh1
    gctx_ref[...] = mm_t(gh1.astype(bf16), w2_ref[:, :D]).astype(bf16)


def ffn(lengths, x, ctx, cot, w2, wd, g1, g2, tm=256, cj=768):
    n = x.shape[0]
    row = pl.BlockSpec((tm, D), lambda i, *_: (i, 0))
    full = lambda a: pl.BlockSpec(a.shape, lambda i, *_: (0, 0), pipeline_mode=pl.Buffered(1))
    sd = jax.ShapeDtypeStruct
    return pl.pallas_call(
        functools.partial(ffn_kernel, tm, cj),
        grid_spec=pltpu.PrefetchScalarGridSpec(
            num_scalar_prefetch=1, grid=(n // tm,),
            in_specs=[row, row, row, full(w2), full(wd), full(g1), full(g2)],
            out_specs=[row, row, row],
            scratch_shapes=[pltpu.VMEM((FF // cj, tm, cj), bf16), pltpu.VMEM((tm, D), f32)]),
        out_shape=[sd((n, D), bf16), sd((n, D), f32), sd((n, D), bf16)],
        name="ffn",
        compiler_params=vm(56),
    )(lengths, x, ctx, cot, w2, wd, g1, g2)


def attn_bwd_kernel(q_ref, k_ref, v_ref, ctx_ref, gc_ref, p_ref, gq_ref, gk_ref, gv_ref):
    lane = lax.broadcasted_iota(jnp.int32, (L, 2 * HD), 1)
    q = q_ref[...]
    k = k_ref[...]
    v = v_ref[...]
    gc = gc_ref[...]
    zero = jnp.zeros_like(k)
    prod = (gc.astype(f32) * ctx_ref[...].astype(f32)).T
    kt = k.T
    gq_parts = []
    gk = jnp.zeros((L, 2 * HD), f32)
    gv = jnp.zeros((L, 2 * HD), f32)
    for h in range(2):
        mine = (lane // HD) == h
        vh = jnp.where(mine, v, zero)
        qh = jnp.where(mine, q, zero)
        gch = jnp.where(mine, gc, zero)
        pt = p_ref[h]
        gpt = mm_t(vh, gc)
        row = jnp.sum(prod[h * HD:(h + 1) * HD], axis=0, keepdims=True)
        gst = (pt.astype(f32) * (gpt - row)).astype(bf16)
        gq_parts.append(mm(kt[h * HD:(h + 1) * HD], gst))
        gk += mm(gst, qh)
        gv += mm(pt, gch)
    gq = jnp.concatenate(gq_parts, axis=0) * (HD ** -0.5)
    gq_ref[...] = gq.astype(bf16).T
    gk_ref[...] = gk.astype(bf16)
    gv_ref[...] = gv.astype(bf16)


def attn_bwd(q, k, v, ctx, gc, p):
    n = q.shape[0]
    seqs = n // L
    pairs = H // 2
    blk = pl.BlockSpec((L, 2 * HD), lambda s, h: (s, h))
    sd = jax.ShapeDtypeStruct
    return pl.pallas_call(
        attn_bwd_kernel,
        grid=(seqs, pairs),
        in_specs=[blk] * 5 + [pl.BlockSpec((2, L, L), lambda s, h: (s * pairs + h, 0, 0))],
        out_specs=[blk] * 3,
        out_shape=[sd((n, D), bf16)] * 3,
        name="attn_bwd",
        compiler_params=vm(48),
    )(q, k, v, ctx, gc, p)


def grads_kernel(gq_ref, gk_ref, gv_ref, dq_ref, dv_ref, ra_ref, gh1_ref, w1_ref, b_ref,
                 qd_ref, vd_ref, qb_ref, vb_ref, gt_ref, sqd_ref, svd_ref, sqb_ref, svb_ref):
    i = pl.program_id(0)

    @pl.when(i == 0)
    def _():
        for ref in (sqd_ref, svd_ref, sqb_ref, svb_ref):
            ref[...] = jnp.zeros_like(ref)

    gq = gq_ref[...].astype(f32)
    gv = gv_ref[...].astype(f32)
    ra = ra_ref[...].astype(f32)
    sqb_ref[...] += fold8(gq * dq_ref[...].astype(f32))
    svb_ref[...] += fold8(gv * dv_ref[...].astype(f32))
    t_q = mm_t((qb_ref[...] * gq).astype(bf16), b_ref[...])
    t_v = mm_t((vb_ref[...] * gv).astype(bf16), b_ref[...])
    sqd_ref[...] += fold8(t_q * ra)
    svd_ref[...] += fold8(t_v * ra)
    g_rank = (t_q * qd_ref[...] + t_v * vd_ref[...]).astype(bf16)
    acc = gh1_ref[...].astype(f32)
    acc += mm_t(gq_ref[...], w1_ref[:, R:R + D])
    acc += mm_t(gk_ref[...], w1_ref[:, R + D:R + 2 * D])
    acc += mm_t(gv_ref[...], w1_ref[:, R + 2 * D:])
    acc += mm_t(g_rank, w1_ref[:, :R])
    gt_ref[...] = acc.astype(bf16)


def grads(gq, gk, gv, dq, dv, ra, gh1, w1, b, qd, vd, qb, vb, tm=256):
    n = gq.shape[0]
    row = lambda c: pl.BlockSpec((tm, c), lambda i: (i, 0))
    full = lambda a: pl.BlockSpec(a.shape, lambda i: (0, 0), pipeline_mode=pl.Buffered(1))
    acc = lambda c: pl.BlockSpec((8, c), lambda i: (0, 0))
    sd = jax.ShapeDtypeStruct
    return pl.pallas_call(
        grads_kernel,
        grid=(n // tm,),
        in_specs=[row(D)] * 5 + [row(R), row(D), full(w1), full(b)] + [full(a) for a in (qd, vd, qb, vb)],
        out_specs=[row(D), acc(R), acc(R), acc(D), acc(D)],
        out_shape=[sd((n, D), bf16), sd((8, R), f32), sd((8, R), f32), sd((8, D), f32), sd((8, D), f32)],
        name="grads",
        compiler_params=vm(48),
    )(gq, gk, gv, dq, dv, ra, gh1, w1, b, qd, vd, qb, vb)


MESH = pl.DeviceIdType.MESH
N_COPIES = 31


def flip(i, bit):
    if bit == 0:
        return i
    if bit == 1:
        return i + 1 - 2 * lax.rem(i, 2)
    if bit == 2:
        return lax.rem(i + 2, 4)
    return 3 - i


class Gather:
    def __init__(self, srcs, dsts, send, recv, local):
        self.srcs, self.dsts, self.send, self.recv, self.local = srcs, dsts, send, recv, local
        dp = lax.axis_index("dp")
        self.z = lax.axis_index("fsdp")
        self.core = lax.rem(dp, 2)
        self.chip = dp // 2

    def peers(self):
        chip, core, z = self.chip, self.core, self.z
        out = [(chip * 2 + 1 - core, z), (flip(chip, 1) * 2 + core, z), (flip(chip, 2) * 2 + core, z)]
        return out + [(chip * 2 + core, flip(z, j)) for j in (1, 2, 3)]

    def barrier(self):
        sem = pltpu.get_barrier_semaphore()
        for peer in self.peers():
            pl.semaphore_signal(sem, inc=1, device_id=peer, device_id_type=MESH)
        pl.semaphore_wait(sem, 6)

    def block(self, a, k, j, core):
        rows = self.srcs[a].shape[0]
        at = ((flip(self.chip, k) * 2 + core) * 4 + flip(self.z, j)) * rows
        return self.dsts[a].at[pl.ds(pl.multiple_of(at, 8), rows), :]

    def z_route(self, j):
        return j - 1, 0, j, (self.chip * 2 + self.core, flip(self.z, j))

    def side_route(self, axis, j):
        peer = (flip(self.chip, axis) * 2 + self.core, self.z)
        return 3 + 4 * (axis - 1) + j, axis, j, peer

    def far_route(self, j):
        axis = 2 if j % 2 == 0 else 1
        return 11 + j, 3, j, (flip(self.chip, axis) * 2 + self.core, self.z)

    def pair_route(self, k, j):
        return 15 + 4 * k + j, k, j, (self.chip * 2 + 1 - self.core, self.z)

    def copy(self, a, route, src, dst):
        key, _, _, peer = route
        return pltpu.make_async_remote_copy(
            src_ref=src, dst_ref=dst, send_sem=self.send.at[a, key], recv_sem=self.recv.at[a, key],
            device_id=peer, device_id_type=MESH)

    def start(self, route, k, j, own=False):
        for a in range(len(self.srcs)):
            here = self.block(a, k, j, self.core)
            self.copy(a, route, self.srcs[a] if own else here, here).start()

    def arrive(self, route):
        _, k, j, _ = route
        for a in range(len(self.srcs)):
            core = 1 - self.core if route[0] >= 15 else self.core
            here = self.block(a, k, j, core)
            self.copy(a, route, here, here).wait_recv()

    def keep_own(self, a):
        return pltpu.make_async_copy(self.srcs[a], self.block(a, 0, 0, self.core), self.local.at[a])

    def first(self):
        for axis in (1, 2):
            self.start(self.side_route(axis, 0), 0, 0, own=True)
        for j in (1, 2, 3):
            self.start(self.z_route(j), 0, 0, own=True)
        self.start(self.pair_route(0, 0), 0, 0, own=True)
        for a in range(len(self.srcs)):
            self.keep_own(a).start()

    def take_z(self, j):
        self.arrive(self.z_route(j))
        for axis in (1, 2):
            self.start(self.side_route(axis, j), 0, j)
        self.start(self.pair_route(0, j), 0, j)

    def take_side(self, axis, j):
        self.arrive(self.side_route(axis, j))
        if axis == (1 if j % 2 == 0 else 2):
            self.start(self.far_route(j), axis, j)
        self.start(self.pair_route(axis, j), axis, j)

    def take_far(self, j):
        self.arrive(self.far_route(j))
        self.start(self.pair_route(3, j), 3, j)

    def last(self):
        for k in range(4):
            for j in range(4):
                self.arrive(self.pair_route(k, j))
        for a in range(len(self.srcs)):
            self.keep_own(a).wait()
            for j in (1, 2, 3):
                self.done(a, self.z_route(j))
            for j in range(4):
                for axis in (1, 2):
                    self.done(a, self.side_route(axis, j))
                self.done(a, self.far_route(j))
                for k in range(4):
                    self.done(a, self.pair_route(k, j))

    def done(self, a, route):
        here = self.block(a, 0, 0, self.core)
        self.copy(a, route, here, here).wait_send()

    def events(self):
        z = lambda j: functools.partial(self.take_z, j)
        s = lambda axis, j: functools.partial(self.take_side, axis, j)
        d = lambda j: functools.partial(self.take_far, j)
        return [self.barrier, self.first, s(1, 0), s(2, 0), z(1), z(2), s(1, 1), s(2, 1), z(3), d(0), s(1, 2), s(2, 2),
                d(1), s(1, 3), s(2, 3), d(2), d(3), self.last]


def gather_scratch(n):
    return [pltpu.SemaphoreType.DMA((n, N_COPIES)), pltpu.SemaphoreType.DMA((n, N_COPIES)),
            pltpu.SemaphoreType.DMA((n,))]


def gather_kernel(n, *refs):
    g = Gather(refs[:n], refs[n:2 * n], *refs[2 * n:])
    for event in g.events():
        event()


def gather(arrays, collective_id):
    axes = ("dp", "fsdp")
    n_dp, n_z = lax.axis_size("dp"), lax.axis_size("fsdp")
    if (n_dp, n_z) != (8, 4) or any(a.shape[0] % 8 for a in arrays):
        return [lax.all_gather(a, axes, axis=0, tiled=True) for a in arrays]
    n = len(arrays)
    whole = [jax.ShapeDtypeStruct((a.shape[0] * n_dp * n_z,) + a.shape[1:], a.dtype) for a in arrays]
    spec = pl.BlockSpec(memory_space=pl.ANY)
    return pl.pallas_call(
        functools.partial(gather_kernel, n),
        in_specs=[spec] * n,
        out_specs=[spec] * n,
        out_shape=whole,
        scratch_shapes=gather_scratch(n),
        name="gather",
        compiler_params=pltpu.CompilerParams(collective_id=collective_id, has_side_effects=True),
    )(*arrays)


def total_kernel(n_z, n_chip, len_ref, sqd_ref, svd_ref, sq_ref, sqb_ref, svb_ref,
                 qd_out, qb_out, vd_out, vb_out, stat_out,
                 mine, pair, line, plane, sends, pair_sem, line_sem, plane_sem):
    dp, z = lax.axis_index("dp"), lax.axis_index("fsdp")
    core, chip = lax.rem(dp, 2), dp // 2
    partner = (chip * 2 + 1 - core, z)
    lines = [(dp, lax.rem(z + j, n_z)) for j in range(1, n_z)]
    planes = [(lax.rem(chip + j, n_chip) * 2 + core, z) for j in range(1, n_chip)]
    sem = pltpu.get_barrier_semaphore()
    for peer in [partner] + lines + planes:
        pl.semaphore_signal(sem, inc=1, device_id=peer, device_id_type=MESH)

    mine[...] = jnp.zeros_like(mine)
    for row, ref in enumerate((sqd_ref, svd_ref, sq_ref, sqb_ref, svb_ref)):
        mine[row:row + 1, :ref.shape[1]] = jnp.sum(ref[...], axis=0, keepdims=True)
    count = len_ref[0]
    for s in range(1, len_ref.shape[0]):
        count += len_ref[s]
    mine[5:6, :] = jnp.full((1, R), count.astype(f32))
    pl.semaphore_wait(sem, n_z + n_chip - 1)

    def send(src, dst, at, recv, peer):
        return pltpu.make_async_remote_copy(
            src_ref=src, dst_ref=dst, send_sem=sends.at[at], recv_sem=recv, device_id=peer, device_id_type=MESH)

    swap = send(mine, pair, 0, pair_sem, partner)
    swap.start()
    swap.wait_recv()
    line[z] = mine[...] + pair[...]
    out = [send(line.at[z], line.at[z], j, line_sem.at[j - 1], lines[j - 1]) for j in range(1, n_z)]
    for copy in out:
        copy.start()
    for j in range(1, n_z):
        came = lax.rem(z + n_z - j, n_z)
        send(line.at[came], line.at[came], j, line_sem.at[j - 1], lines[j - 1]).wait_recv()
    total = line[0]
    for i in range(1, n_z):
        total += line[i]
    plane[chip] = total
    far = [send(plane.at[chip], plane.at[chip], n_z - 1 + j, plane_sem.at[j - 1], planes[j - 1])
           for j in range(1, n_chip)]
    for copy in far:
        copy.start()
    for j in range(1, n_chip):
        came = lax.rem(chip + n_chip - j, n_chip)
        send(plane.at[came], plane.at[came], n_z - 1 + j, plane_sem.at[j - 1], planes[j - 1]).wait_recv()
    total = plane[0]
    for i in range(1, n_chip):
        total += plane[i]
    qd_out[...] = total[0:1]
    vd_out[...] = total[1:2]
    stat_out[...] = total[2:3] / total[5:6]
    qb_out[...] = total[3:4, :D]
    vb_out[...] = total[4:5, :D]
    for copy in [swap] + out + far:
        copy.wait_send()


def total(lengths, s_qd, s_vd, sq, s_qb, s_vb, collective_id):
    n_z = lax.axis_size("fsdp")
    n_chip = lax.axis_size("dp") // 2
    vmem = pl.BlockSpec(memory_space=pltpu.VMEM)
    sd = jax.ShapeDtypeStruct
    dma = pltpu.SemaphoreType.DMA
    return pl.pallas_call(
        functools.partial(total_kernel, n_z, n_chip),
        in_specs=[pl.BlockSpec(memory_space=pltpu.SMEM)] + [vmem] * 5,
        out_specs=[vmem] * 5,
        out_shape=[sd((1, R), f32), sd((1, D), f32), sd((1, R), f32), sd((1, D), f32), sd((1, R), f32)],
        scratch_shapes=[pltpu.VMEM((8, R), f32), pltpu.VMEM((8, R), f32), pltpu.VMEM((n_z, 8, R), f32),
                        pltpu.VMEM((n_chip, 8, R), f32), dma((n_z + n_chip - 1,)), dma(()), dma((n_z - 1,)),
                        dma((n_chip - 1,))],
        name="total",
        compiler_params=pltpu.CompilerParams(collective_id=collective_id, has_side_effects=True),
    )(lengths, s_qd, s_vd, sq, s_qb, s_vb)


def shards(
    tokens,
    lengths,
    cotangent,
    w_query,
    w_key,
    w_value,
    w_out,
    w_up,
    w_down,
    shared_a,
    shared_b,
    gain_one,
    gain_two,
    query_d,
    query_b,
    value_d,
    value_b,
):
    seqs = tokens.shape[0]
    x = tokens.reshape(seqs * L, D)
    cot = cotangent.reshape(seqs * L, D)
    w1, b, w2, wd = gather(
        (
            jnp.concatenate([shared_a, w_query, w_key, w_value], axis=1),
            shared_b,
            jnp.concatenate([w_out, w_up], axis=1),
            w_down,
        ),
        0,
    )
    g1, g2, qd, qb, vd, vb = (
        a.reshape(1, -1) for a in (gain_one, gain_two, query_d, query_b, value_d, value_b)
    )
    ra, dq, dv, q, k, v, sq = proj(lengths, x, w1, b, qd, vd, qb, vb)
    ctx, p = attn_fwd(lengths, q, k, v)
    out, gh1, gc = ffn(lengths, x, ctx, cot, w2, wd, g1, g2)
    gq, gk, gv = attn_bwd(q, k, v, ctx, gc, p)
    gt, s_qd, s_vd, s_qb, s_vb = grads(gq, gk, gv, dq, dv, ra, gh1, w1, b, qd, vd, qb, vb)
    sums = total(lengths, s_qd, s_vd, sq, s_qb, s_vb, 1)
    return (out.reshape(seqs, L, D), gt.reshape(seqs, L, D)) + tuple(a.reshape(-1) for a in sums)


def solution(mesh):
    from jax.sharding import PartitionSpec as P

    both = ("dp", "fsdp")
    mat = P(both, None)
    big = P(both, None, None)
    in_specs = (big, P(both), big) + (mat,) * 8 + (P(),) * 6
    out_specs = (big, big) + (P(),) * 5
    return jax.shard_map(shards, mesh=mesh, in_specs=in_specs, out_specs=out_specs, check_vma=False)
```
